128 devices in a mesh: prow: 8 (over x_lo, z), pcol: 16 (over y, x_hi, core).
Axes of the slice: x: 4 (x_hi: 2, x_lo: 2; x = x_hi * 2 + x_lo), y: 4, z: 4, core: 2. Of those that a mesh axis runs over, the one named last changes fastest.
Arguments:
- pool_inverse: bfloat16 [24576, 24576], P('pcol', 'prow'), may hold values from -6 to 6
- list_a: int32 [32], replicated, may hold values from 0 to 95, as said below
- list_b: int32 [29], replicated, may hold values from 0 to 95, as said below
- fact_a: bfloat16 [8192, 768], P('pcol'), may hold values from -0.0625 to 0.0625
- fact_b: bfloat16 [7424, 768], P('pcol'), may hold values from -0.0625 to 0.0625
- fact_b_anc: bfloat16 [768, 768], P('prow'), may hold values from -0.21875 to 0.21875
- dinv_a: float32 [768, 768], P('prow'), may hold values from -6 to 6
- dinv_b: float32 [768, 768], P('prow'), may hold values from -6 to 6
Outputs:
- sel_a: float32 [24576, 768], P('pcol', 'prow')
- sigma_aa: float32 [768, 768], P('prow')
- sel_b: float32 [24576, 768], P('pcol', 'prow')
- sel_b_anc: float32 [768, 768], P('prow')
- sigma_bb: float32 [768, 768], P('prow')
The draws below stay inside these ranges and needn't reach their ends.
Inputs may be any that keep to these rules, and one draw needn't show every extreme that they name: `list_a`: distinct and ascending. `list_b`: distinct and ascending, every entry also in list_a; it holds the block rows 0, 6 and 48.
All inputs are finite; a program needn't handle non-finite values.
Results may differ from the reference program's by a relative error of at most 0.0003.
Values may be sent and summed in bfloat16 or wider, within the bound.
A program may use at most 192 MiB of HBM per device.

```python
import jax
import jax.numpy as jnp
from jax import lax

W = 768
BS = 256
NLA = 32
NPOOL = 96
NLB = 29
N_PCOL = 16


def forced_flag(values):
    second = NPOOL // N_PCOL
    middle = NPOOL // 2
    return (values == 0) | (values == second) | (values == middle)


def both_lists(key):
    shuffled = jax.random.permutation(jax.random.fold_in(key, 17), NPOOL).astype(jnp.int32)
    blocks = jnp.arange(NPOOL, dtype=jnp.int32)
    position = jnp.zeros((NPOOL,), jnp.int32).at[shuffled].set(blocks)
    scores_a = position - NPOOL * forced_flag(blocks).astype(jnp.int32)
    order_a = jnp.argsort(scores_a, stable=True).astype(jnp.int32)
    listed_a = jnp.sort(order_a[:NLA]).astype(jnp.int32)
    picks = jax.random.permutation(jax.random.fold_in(key, 29), NLA).astype(jnp.int32)
    slots = jnp.arange(NLA, dtype=jnp.int32)
    rank_b = jnp.zeros((NLA,), jnp.int32).at[picks].set(slots)
    scores_b = rank_b - NLA * forced_flag(listed_a).astype(jnp.int32)
    order_b = jnp.argsort(scores_b, stable=True).astype(jnp.int32)
    listed_b = jnp.sort(listed_a[order_b[:NLB]]).astype(jnp.int32)
    return (listed_a, listed_b)


def draw_list_a(key, part):
    return both_lists(key)[0]


def draw_list_b(key, part):
    return both_lists(key)[1]


def shard_levels(own_key, shape, split, smallest, largest):
    def one(dim, parts):
        heights = jax.random.uniform(jax.random.fold_in(jax.random.fold_in(own_key, 6), dim), (parts,), jnp.float32, smallest / len(split), largest / len(split))
        return jnp.repeat(jnp.exp(heights), shape[dim] // parts).reshape((-1,) + (1,) * (len(shape) - dim - 1))

    gain = one(*split[0])
    for cut in split[1:]:
        gain = gain * one(*cut)
    return gain


def centred(rng, extent, width, bound, split=(), kind=jnp.bfloat16):
    array = jax.random.normal(rng, extent, jnp.float32) * width
    if len(split) > 0:
        array = shard_levels(rng, extent, split, -0.22, 0.18) * array
    return jnp.clip(array, min=-bound, max=bound).astype(kind)


def setup_inputs(seed: int = 0) -> dict:
    splits = jax.random.split(jax.random.key(seed), 9)
    return {
        "pool_inverse": centred(splits[0], (NPOOL * BS, NPOOL * BS), 1.0, 6.0, ((0, 16), (1, 8))),
        "list_a": draw_list_a(jax.random.fold_in(splits[8], 71), 0),
        "list_b": draw_list_b(jax.random.fold_in(splits[8], 71), 0),
        "fact_a": centred(splits[3], (NLA * BS, W), (NLA * BS) ** -0.5, 0.0625, ((0, 16),)),
        "fact_b": centred(splits[4], (NLB * BS, W), (NLA * BS) ** -0.5, 0.0625, ((0, 16),)),
        "fact_b_anc": centred(splits[5], (W, W), W ** -0.5, 0.21875, ((0, 8),)),
        "dinv_a": centred(splits[6], (W, W), 1.0, 6.0, ((0, 8),), jnp.float32),
        "dinv_b": centred(splits[7], (W, W), 1.0, 6.0, ((0, 8),), jnp.float32),
    }


def blocks_of(pool, rows, cols):
    tiles = pool.reshape(NPOOL, BS, NPOOL, BS)
    picked = jnp.take(jnp.take(tiles, rows, axis=0), cols, axis=2)
    return picked.reshape(rows.shape[0] * BS, cols.shape[0] * BS)


def spread_rows(listed, listing):
    count = listing.shape[0]
    filled = jnp.zeros((NPOOL, BS, W), jnp.float32).at[listing].set(listed.reshape(count, BS, W))
    return filled.reshape(NPOOL * BS, W)


def reference(pool_inverse, list_a, list_b, fact_a, fact_b, fact_b_anc, dinv_a, dinv_b):
    highest = lax.Precision.HIGHEST
    fa32 = fact_a.astype(jnp.float32)
    fb32 = fact_b.astype(jnp.float32)
    anc32 = fact_b_anc.astype(jnp.float32)
    xa_list = -jnp.dot(blocks_of(pool_inverse, list_a, list_a), fact_a, preferred_element_type=jnp.float32)
    sel_a = spread_rows(xa_list, list_a)
    sigma_aa = dinv_a + jnp.dot(xa_list.T, fa32, precision=highest)
    xa_on_b = jnp.take(sel_a.reshape(NPOOL, BS, W), list_b, axis=0).reshape(NLB * BS, W)
    y_bp = jnp.dot(blocks_of(pool_inverse, list_b, list_b), fact_b, preferred_element_type=jnp.float32)
    y_bp = y_bp + jnp.dot(xa_on_b, anc32, precision=highest)
    xb_list = -y_bp
    sel_b = spread_rows(xb_list, list_b)
    sel_b_anc = -(jnp.dot(xa_on_b.T, fb32, precision=highest) + jnp.dot(sigma_aa, anc32, precision=highest))
    sigma_bb = dinv_b + jnp.dot(xb_list.T, fb32, precision=highest) + jnp.dot(sel_b_anc.T, anc32, precision=highest)
    return sel_a, sigma_aa, sel_b, sel_b_anc, sigma_bb
```

```python
import functools

import jax
import jax.numpy as jnp
from jax import lax
from jax.experimental import pallas as pl
from jax.experimental.pallas import tpu as pltpu
from jax.sharding import PartitionSpec as P

BS = 256
HIGHEST = lax.Precision.HIGHEST
SIZES = ((3, 6), (4, 6), (4, 8), (5, 8), (6, 12))


def exchange(x, axis):
    return lax.all_to_all(x, axis, split_axis=0, concat_axis=0, tiled=True)


def sent_to_all(x, axis):
    copies = jnp.broadcast_to(x, (lax.axis_size(axis), *x.shape))
    return exchange(copies, axis)


def product_kernel(rows, steps, width, row_ids, col_ids, pool_ref, u_ref, anc_ref, out_ref, total):
    step = pl.program_id(0)

    @pl.when(step == 0)
    def _():
        total[...] = jnp.zeros_like(total)

    u = u_ref[...].reshape(BS, 2 * width)

    def add(k, carry):
        first = pl.multiple_of(row_ids[k] * BS, BS)
        total[k] += jnp.dot(pool_ref[pl.ds(first, BS), :], u, preferred_element_type=jnp.float32)
        return carry

    lax.fori_loop(0, rows, add, 0)

    @pl.when(step == steps - 1)
    def _():
        anc = anc_ref[...]

        def finish(k, carry):
            own = total[k, :, :width]
            high = own.astype(jnp.bfloat16)
            low = (own - high.astype(jnp.float32)).astype(jnp.bfloat16)
            term = jnp.dot(high, anc, preferred_element_type=jnp.float32)
            term = term + jnp.dot(low, anc, preferred_element_type=jnp.float32)
            other = total[k, :, width:] - term
            at = pl.ds(pl.multiple_of(k * BS, BS), BS)
            out_ref[0, :, at] = own.T
            out_ref[1, :, at] = other.T
            return carry

        lax.fori_loop(0, rows, finish, 0)


def products(pool, row_ids, col_ids, u, anc):
    pieces, steps, depth, width2 = u.shape
    rows = row_ids.shape[0]
    width = width2 // 2
    grid_spec = pltpu.PrefetchScalarGridSpec(
        num_scalar_prefetch=2,
        grid=(steps,),
        in_specs=[
            pl.BlockSpec((pool.shape[0], BS), lambda m, ri, ci: (0, ci[m])),
            pl.BlockSpec((pieces, None, depth, width2), lambda m, ri, ci: (0, m, 0, 0)),
            pl.BlockSpec(anc.shape, lambda m, ri, ci: (0, 0)),
        ],
        out_specs=pl.BlockSpec((2, width, rows * BS), lambda m, ri, ci: (0, 0, 0)),
        scratch_shapes=[pltpu.VMEM((rows, BS, width2), jnp.float32)],
    )
    flops = 2 * rows * BS * width2 * (steps * BS + width)
    return pl.pallas_call(
        functools.partial(product_kernel, rows, steps, width),
        grid_spec=grid_spec,
        out_shape=jax.ShapeDtypeStruct((2, width, rows * BS), jnp.float32),
        compiler_params=pltpu.CompilerParams(
            dimension_semantics=("arbitrary",), vmem_limit_bytes=60 * 1024 * 1024
        ),
        cost_estimate=pl.CostEstimate(
            flops=flops, bytes_accessed=2 * u.size + 4 * 2 * width * rows * BS, transcendentals=0
        ),
        name="products",
    )(row_ids, col_ids, pool, u, anc)


def piece_slots(ids, valid, list_a, list_b, piece, pcol):
    at_a = jnp.sum((list_a < ids[..., None]).astype(jnp.int32), axis=-1)
    at_b = jnp.sum((list_b < ids[..., None]).astype(jnp.int32), axis=-1)
    in_b = valid & jnp.any(list_b == ids[..., None], axis=-1)
    held_b = list_b.shape[0]
    group = at_b * pcol + piece
    slot_a = (at_a // 2) * 4 + at_a % 2
    slot_b = (group // held_b) * 4 + 2 + (group % held_b) // pcol
    return slot_a, slot_b, in_b


def chosen(pieces, slots, valid):
    slot_a, slot_b, in_b = slots
    part_a = jnp.take(pieces, slot_a, axis=0, mode="clip")
    part_a = jnp.where(valid[..., None, None], part_a, 0)
    part_b = jnp.take(pieces, slot_b, axis=0, mode="clip")
    part_b = jnp.where(in_b[..., None, None], part_b, 0)
    return jnp.concatenate([part_a, part_b], axis=-1)


def ids_of(list_a, first, span, count):
    padded = jnp.concatenate([list_a, jnp.full((count,), 4096, jnp.int32)])
    start = jnp.sum((list_a < first[..., None]).astype(jnp.int32), axis=-1)
    ids = jnp.take(padded, start[..., None] + jnp.arange(count, dtype=jnp.int32), axis=0)
    return ids, ids < first[..., None] + span


def main_part(rows, cols, pool, list_a, list_b, pieces, anc):
    pcol, prow = lax.axis_size("pcol"), lax.axis_size("prow")
    col_index, row_index = lax.axis_index("pcol"), lax.axis_index("prow")
    row_span, col_span = pool.shape[0] // BS, pool.shape[1] // BS
    width = pieces.shape[-1]
    depth = pieces.shape[-2]
    first = row_index * col_span
    ids, valid = ids_of(list_a, first, col_span, cols)
    mine = chosen(pieces, piece_slots(ids, valid, list_a, list_b, col_index, pcol), valid)
    u_cols = lax.all_gather(mine, "pcol", axis=0)
    firsts = jnp.arange(pcol, dtype=jnp.int32) * row_span
    ids_all, valid_all = ids_of(list_a, firsts, row_span, rows)
    slots_all = piece_slots(ids_all, valid_all, list_a, list_b, col_index, pcol)
    sends = chosen(pieces, slots_all, valid_all)
    u_rows = exchange(sends, "pcol")
    u_rows = jnp.moveaxis(u_rows, 0, 1).reshape(rows * BS, 2 * width)
    own_ids = jnp.take(ids_all, col_index, axis=0)
    own_valid = jnp.take(valid_all, col_index, axis=0)
    own_first = col_index * row_span
    row_ids = jnp.clip(own_ids - own_first, 0, row_span - 1)
    col_ids = jnp.clip(ids - first, 0, col_span - 1)
    part = products(pool, row_ids, col_ids, u_cols, anc)
    summed = lax.psum_scatter(part, "prow", scatter_dimension=1, tiled=True)
    own_b = own_valid & jnp.any(list_b == own_ids[:, None], axis=-1)
    keep = jnp.stack([own_valid, own_b]).astype(jnp.float32)
    sel = -summed.reshape(2, -1, rows, BS) * keep[:, None, :, None]
    flat = sel.reshape(2, -1, rows * BS)
    u_rows = u_rows.astype(jnp.float32)
    first_part = jnp.dot(flat[0], u_rows, precision=HIGHEST)
    second_part = jnp.dot(flat[1], u_rows[:, width:], precision=HIGHEST)
    total = jnp.concatenate([first_part, second_part], axis=1)
    wanted = own_first + jnp.arange(row_span, dtype=jnp.int32)
    rank = jnp.sum((own_ids < wanted[:, None]).astype(jnp.int32), axis=1)
    listed = jnp.any(own_ids == wanted[:, None], axis=1).astype(jnp.float32)
    spread = jnp.take(sel, rank, axis=2, mode="clip") * listed[None, None, :, None]
    spread = spread.reshape(2, -1, row_span * BS)
    return total, spread[0].T, spread[1].T


def per_device(pool_inverse, list_a, list_b, fact_a, fact_b, fact_b_anc, dinv_a, dinv_b):
    pcol, prow = lax.axis_size("pcol"), lax.axis_size("prow")
    col_index, row_index = lax.axis_index("pcol"), lax.axis_index("prow")
    width = fact_a.shape[1]
    part_width = fact_b_anc.shape[0]
    depth = BS // pcol
    own_a = fact_a.reshape(-1, pcol, depth, width)
    held_b = fact_b.shape[0] // depth
    own_b = jnp.pad(fact_b.reshape(held_b, depth, width), ((0, 2 * pcol - held_b), (0, 0), (0, 0)))
    own_b = own_b.reshape(2, pcol, depth, width)
    shift = (held_b * col_index) % pcol
    own_b = lax.dynamic_slice_in_dim(
        jnp.concatenate([own_b, own_b], axis=1), (pcol - shift) % pcol, pcol, axis=1
    )
    sends = jnp.moveaxis(jnp.concatenate([own_a, own_b], axis=0), 0, 1)
    pieces = exchange(sends, "pcol").reshape(-1, depth, width)
    anc = sent_to_all(fact_b_anc, "prow").reshape(-1, width)
    row_span, col_span = pool_inverse.shape[0] // BS, pool_inverse.shape[1] // BS
    per_row = jnp.sum((list_a // row_span == jnp.arange(pcol)[:, None]).astype(jnp.int32), axis=1)
    per_col = jnp.sum((list_a // col_span == jnp.arange(prow)[:, None]).astype(jnp.int32), axis=1)
    most_rows, most_cols = jnp.max(per_row), jnp.max(per_col)
    fits = [(most_rows <= rows) & (most_cols <= cols) for rows, cols in SIZES]
    choice = jnp.int32(len(SIZES) - 1)
    for i in reversed(range(len(SIZES) - 1)):
        choice = jnp.where(fits[i], i, choice)
    branches = [functools.partial(main_part, rows, cols) for rows, cols in SIZES]
    total, sel_a, sel_b = lax.switch(
        choice, branches, pool_inverse, list_a, list_b, pieces, anc
    )
    anc32 = anc.astype(jnp.float32)
    each = total.shape[0] // pcol
    total = total.reshape(pcol, each, total.shape[1])
    mine = jnp.sum(exchange(total, "pcol").reshape(total.shape), axis=0)
    total = sent_to_all(mine, "pcol").reshape(part_width, -1)
    sigma_aa = dinv_a + total[:, :width]
    sel_b_anc = -(total[:, width : 2 * width] + jnp.dot(sigma_aa, anc32, precision=HIGHEST))
    sends = jnp.moveaxis(sel_b_anc.reshape(part_width, prow, part_width), 1, 0)
    cross = exchange(sends, "prow").reshape(-1, part_width)
    sigma_bb = dinv_b + total[:, 2 * width :] + jnp.dot(cross.T, anc32, precision=HIGHEST)
    return (sel_a, sigma_aa, sel_b, sel_b_anc, sigma_bb)


def solution(mesh):
    in_specs = (
        P("pcol", "prow"),
        P(),
        P(),
        P("pcol", None),
        P("pcol", None),
        P("prow", None),
        P("prow", None),
        P("prow", None),
    )
    out_specs = (
        P("pcol", "prow"),
        P("prow", None),
        P("pcol", "prow"),
        P("prow", None),
        P("prow", None),
    )
    return jax.shard_map(
        per_device, mesh=mesh, in_specs=in_specs, out_specs=out_specs, check_vma=False
    )
```
